32 devices in a mesh: bank: 8 (over z, core), zero: 4 (over y, x).
Axes of the slice: x: 2, y: 2, z: 4, core: 2. Of those that a mesh axis runs over, the one named last changes fastest.
Arguments:
- master_gate: float32 [64, 2048, 1408], P('bank', 'zero'), may hold values from -0.1875 to 0.1875
- master_up: float32 [64, 2048, 1408], P('bank', 'zero'), may hold values from -0.1875 to 0.1875
- master_down: float32 [64, 1408, 2048], P('bank', None, 'zero'), may hold values from -0.21875 to 0.21875
- router_weight: float32 [2048, 64], P('zero', 'bank'), may hold values from -0.125 to 0.125
- router_gain: float32 [2048], P('zero'), may hold values from 0.25 to 1.75
Outputs:
- final_gate: bfloat16 [64, 2048, 1408], P('bank', None, 'zero')
- final_up: bfloat16 [64, 2048, 1408], P('bank', None, 'zero')
- final_down: bfloat16 [64, 1408, 2048], P('bank', 'zero')
- scale_gate: float32 [64, 1408], P('bank', 'zero')
- scale_up: float32 [64, 1408], P('bank', 'zero')
- scale_down: float32 [64, 1408], P('bank', 'zero')
- serve_router: bfloat16 [2048, 64], replicated
The draws below stay inside these ranges and needn't reach their ends.
All inputs are finite; a program needn't handle non-finite values. Where the reference program divides by a largest or mean magnitude, that divisor is 1e-20 or more.
Results may differ from the reference program's by a relative error of at most 0.0013.
Values may be sent and summed in bfloat16 or wider, within the bound.
A program may use at most 192 MiB of HBM per device.

```python
import jax
import jax.numpy as jnp

EXPERTS = 64
D_MODEL = 2048
D_EXPERT = 1408


def strengthened(drawn, key, source, target, blocks, factor):
    owner, partner = [(jnp.arange(drawn.shape[axis_at]) // (drawn.shape[axis_at] // blocks)).reshape([-1 if axis == axis_at else 1 for axis in range(drawn.ndim)]) for axis_at in (source, target)]
    chosen = jax.random.permutation(key, blocks)[partner]
    strong = (owner == chosen) | (owner == (partner + blocks // 2) % blocks)
    return jnp.where(strong, factor * drawn, drawn)


def level_of(rng, extent, split, least, high):
    def one(position, parts):
        steps = jax.random.uniform(jax.random.fold_in(jax.random.fold_in(rng, 6), position), (parts,), jnp.float32, least / len(split), high / len(split))
        return jnp.repeat(jnp.exp(steps), extent[position] // parts).reshape((-1,) + (1,) * (len(extent) - position - 1))

    loudness = one(*split[0])
    for cut in split[1:]:
        loudness = loudness * one(*cut)
    return loudness


def normal_values(own_key, dims, width, reach, cuts=(), held_as=jnp.bfloat16):
    values = width * jax.random.normal(own_key, dims, jnp.float32)
    if cuts:
        values = values * level_of(own_key, dims, cuts, -0.22, 0.18)
    return jnp.clip(values, -reach, reach).astype(held_as)


def noise_with(own_key, extent, scale, reach, pieces, heavy, dtype=jnp.bfloat16):
    entries = scale * jax.random.normal(own_key, extent, jnp.float32)
    if pieces:
        entries = entries * level_of(own_key, extent, pieces, -0.22, 0.18)
    return jnp.clip(strengthened(entries, jax.random.fold_in(own_key, 3), *heavy), -reach, reach).astype(dtype)


def setup_inputs(seed: int = 0) -> dict:
    keys = jax.random.split(jax.random.key(seed), 6)
    return {
        "master_gate": noise_with(keys[0], (EXPERTS, D_MODEL, D_EXPERT), D_MODEL ** -0.5, 0.1875, ((0, 8), (1, 4)), (1, 2, 4, 2.0), jnp.float32),
        "master_up": noise_with(keys[1], (EXPERTS, D_MODEL, D_EXPERT), D_MODEL ** -0.5, 0.1875, ((0, 8), (1, 4)), (1, 2, 4, 2.0), jnp.float32),
        "master_down": noise_with(keys[2], (EXPERTS, D_EXPERT, D_MODEL), D_EXPERT ** -0.5, 0.21875, ((0, 8), (2, 4)), (2, 1, 4, 2.0), jnp.float32),
        "router_weight": normal_values(keys[3], (D_MODEL, EXPERTS), D_MODEL ** -0.5, 0.125, ((0, 4), (1, 8)), jnp.float32),
        "router_gain": jnp.clip(1.0 + 0.15 * jax.random.normal(keys[4], (D_MODEL,), jnp.float32), 0.25, 1.75),
    }


def reference(master_gate, master_up, master_down, router_weight, router_gain):
    scale_gate = jnp.sum(jnp.abs(master_gate), axis=1) / D_MODEL
    final_gate = (master_gate / jnp.expand_dims(scale_gate, 1)).astype(jnp.bfloat16)
    scale_up = jnp.sum(jnp.abs(master_up), axis=1) / D_MODEL
    final_up = (master_up / jnp.expand_dims(scale_up, 1)).astype(jnp.bfloat16)
    scale_down = jnp.sum(jnp.abs(master_down), axis=2) / D_MODEL
    final_down = (master_down / jnp.expand_dims(scale_down, 2)).astype(jnp.bfloat16)
    serve_router = (router_weight * router_gain[:, None]).astype(jnp.bfloat16)
    return final_gate, final_up, final_down, scale_gate, scale_up, scale_down, serve_router
```

```python
import functools
import math

import jax
import jax.numpy as jnp
from jax import lax
from jax.experimental import pallas as pl
from jax.experimental.pallas import tpu as pltpu
from jax.sharding import PartitionSpec as P

LANES = 128
DOWN, GATE, UP = range(3)
MESH = pl.DeviceIdType.MESH


def span(index, size):
    return pl.ds(pl.multiple_of(index * size, size), size)


def row_sums_across(wide, put):
    def one(j, _):
        put(j, jnp.sum(jnp.abs(wide[:, span(j, LANES)]), axis=0, keepdims=True))
        return 0

    lax.fori_loop(0, wide.shape[1] // LANES, one, 0)


def row_sums_along(wide, put):
    def one(j, _):
        block = jnp.abs(wide[span(j, LANES), :])
        total = block[:, :LANES]
        for k in range(1, block.shape[1] // LANES):
            total = total + block[:, k * LANES : (k + 1) * LANES]
        put(j, jnp.sum(total.T, axis=0, keepdims=True))
        return 0

    lax.fori_loop(0, wide.shape[0] // LANES, one, 0)


def exchange_kernel(
    parts,
    kept,
    gate,
    up,
    down,
    weight,
    gain,
    out_gate,
    out_up,
    out_down,
    cut,
    out_strip,
    scales,
    wide_gate,
    wide_up,
    wide_down,
    narrow,
    columns_of,
    sums,
    weight_now,
    gain_now,
    strip,
    load_sem,
    sum_send,
    sum_recv,
    data_send,
    data_recv,
    own_sem,
    cut_sem,
    router_load,
    part_send,
    part_recv,
    strip_sem,
):
    me = lax.axis_index("zero")
    experts, rows, inner = gate.shape
    width = inner // parts
    chunk = math.gcd(width, 32)
    d_model = rows * parts
    source = {DOWN: down, GATE: gate, UP: up}
    wide = {DOWN: wide_down, GATE: wide_gate, UP: wide_up}
    result = {DOWN: out_down, GATE: out_gate, UP: out_up}
    peers = [lax.rem(me + k, parts) for k in range(1, parts)]

    def load(m, e):
        slot = lax.rem(e, 2)
        return pltpu.make_async_copy(source[m].at[e], wide[m].at[slot], load_sem.at[m, slot])

    def sum_copy(m, e, k, sender):
        return pltpu.make_async_remote_copy(
            src_ref=sums.at[m, e, sender],
            dst_ref=sums.at[m, e, sender],
            send_sem=sum_send.at[m, k],
            recv_sem=sum_recv.at[m, e, sender],
            device_id={"zero": peers[k]},
            device_id_type=MESH,
        )

    def block_copy(m, e, k, sender):
        slot = lax.rem(e, 2)
        return pltpu.make_async_remote_copy(
            src_ref=narrow.at[m, slot, span(peers[k], width), :],
            dst_ref=result[m].at[e, :, span(sender, rows)],
            send_sem=data_send.at[m, slot, k],
            recv_sem=data_recv.at[m, e, sender],
            device_id={"zero": peers[k]},
            device_id_type=MESH,
        )

    def own_copy(m, e):
        slot = lax.rem(e, 2)
        return pltpu.make_async_copy(
            narrow.at[m, slot, span(me, width), :],
            result[m].at[e, :, span(me, rows)],
            own_sem.at[m, slot],
        )

    def cut_copy(e, p):
        slot = lax.rem(e, 2)
        return pltpu.make_async_copy(
            narrow.at[DOWN, slot, pl.ds(p * width, width), :],
            cut.at[p, e - kept],
            cut_sem.at[slot, p],
        )

    def begin(m, e, ready=lambda: None):
        load(m, e).wait()
        slot = lax.rem(e, 2)
        if m != UP:
            pl.when(e < 2)(lambda: load(m + 1, e).start())
        elif experts > 1:
            pl.when(e < 1)(lambda: load(DOWN, e + 1).start())

        def put(j, value):
            sums[m, e, me, :, span(j, LANES)] = value

        (row_sums_along if m == DOWN else row_sums_across)(wide[m].at[slot], put)
        ready()
        for k in range(parts - 1):
            sum_copy(m, e, k, me).start()

    def sent(m, e):
        def remote():
            for k in range(parts - 1):
                block_copy(m, e, k, me).wait_send()
            own_copy(m, e).wait()

        if m != DOWN:
            remote()
            return
        pl.when(e < kept)(remote)

        @pl.when(e >= kept)
        def _():
            for p in range(parts):
                cut_copy(e, p).wait()

    def finish(m, e):
        slot = lax.rem(e, 2)
        for k in range(parts - 1):
            sum_copy(m, e, k, me).wait_send()
            sum_copy(m, e, k, peers[k]).wait_recv()
        pl.when(e >= 2)(lambda: sent(m, e - 2))
        wide_now, narrow_now = wide[m].at[slot], narrow.at[m, slot]

        def inverse_of(columns):
            total = sums[m, e, 0, :, columns]
            for p in range(1, parts):
                total = total + sums[m, e, p, :, columns]
            scale = total / d_model
            scales[m, e, :, columns] = scale
            return 1.0 / scale

        if m == DOWN:

            def by_row(j, _):
                columns = span(j, LANES)
                inverse = jnp.broadcast_to(inverse_of(columns), (LANES, LANES))
                columns_of[columns, :] = inverse.T
                return 0

            lax.fori_loop(0, inner // LANES, by_row, 0, unroll=True)

            def scaled(p):
                def one(c, _):
                    at = pl.ds(pl.multiple_of(p * width + c * chunk, chunk), chunk)
                    inverse = columns_of[at, :]
                    for i in range(rows // LANES):
                        lanes = pl.ds(i * LANES, LANES)
                        narrow_now[at, lanes] = (wide_now[at, lanes] * inverse).astype(jnp.bfloat16)
                    return 0

                lax.fori_loop(0, width // chunk, one, 0)

            for k in range(parts - 1):
                scaled(peers[k])
                pl.when(e < kept)(lambda: block_copy(DOWN, e, k, me).start())
            scaled(me)
            pl.when(e < kept)(lambda: own_copy(DOWN, e).start())

            @pl.when(e >= kept)
            def _():
                for p in range(parts):
                    cut_copy(e, p).start()

        else:

            def one(j, _):
                columns = span(j, LANES)
                inverse = inverse_of(columns)
                for i in range(rows // LANES):
                    at = pl.ds(i * LANES, LANES)
                    block = wide_now[at, columns] * inverse
                    narrow_now[columns, at] = block.T.astype(jnp.bfloat16)
                return 0

            lax.fori_loop(0, inner // LANES, one, 0)
            for k in range(parts - 1):
                block_copy(m, e, k, me).start()
            own_copy(m, e).start()
        pl.when(e + 2 < experts)(lambda: load(m, e + 2).start())

    def part_copy(k, sender):
        return pltpu.make_async_remote_copy(
            src_ref=strip.at[:, span(sender, rows)],
            dst_ref=strip.at[:, span(sender, rows)],
            send_sem=part_send.at[k],
            recv_sem=part_recv.at[sender],
            device_id={"zero": peers[k]},
            device_id_type=MESH,
        )

    router_loads = [
        pltpu.make_async_copy(weight, weight_now, router_load.at[0]),
        pltpu.make_async_copy(gain, gain_now, router_load.at[1]),
    ]

    load(DOWN, 0).start()
    for copy in router_loads:
        copy.start()
    barrier = pltpu.get_barrier_semaphore()
    for peer in peers:
        pl.semaphore_signal(barrier, inc=1, device_id={"zero": peer}, device_id_type=MESH)
    begin(DOWN, 0, lambda: pl.semaphore_wait(barrier, parts - 1))
    begin(GATE, 0)
    for copy in router_loads:
        copy.wait()
    strip[:, span(me, rows)] = (weight_now[...] * gain_now[...]).astype(jnp.bfloat16)
    for k in range(parts - 1):
        part_copy(k, me).start()

    def step(e, _):
        more = e + 1 < experts
        finish(DOWN, e)
        begin(UP, e)
        pl.when(more)(lambda: begin(DOWN, e + 1))
        finish(GATE, e)
        pl.when(more)(lambda: begin(GATE, e + 1))
        finish(UP, e)
        return 0

    lax.fori_loop(0, experts, step, 0)

    for m in (DOWN, GATE, UP):
        for e in range(max(experts - 2, 0), experts):
            sent(m, jnp.int32(e))

    def arrived(e, _):
        for k in range(parts - 1):
            for m in (GATE, UP):
                block_copy(m, e, k, peers[k]).wait_recv()

            @pl.when(e < kept)
            def _():
                block_copy(DOWN, e, k, peers[k]).wait_recv()

        return 0

    lax.fori_loop(0, experts, arrived, 0)
    for k in range(parts - 1):
        part_copy(k, me).wait_send()
        part_copy(k, peers[k]).wait_recv()
    strip_copy = pltpu.make_async_copy(strip, out_strip, strip_sem)
    strip_copy.start()
    strip_copy.wait()


def exchange(parts, kept, gate, up, down, weight, gain):
    experts, rows, inner = gate.shape
    width, d_model = inner // parts, rows * parts
    left = experts - kept
    any_space = pl.BlockSpec(memory_space=pl.ANY)
    narrow = jnp.bfloat16
    dma = pltpu.SemaphoreType.DMA
    return pl.pallas_call(
        functools.partial(exchange_kernel, parts, kept),
        out_shape=(
            jax.ShapeDtypeStruct((experts, width, d_model), narrow),
            jax.ShapeDtypeStruct((experts, width, d_model), narrow),
            jax.ShapeDtypeStruct((kept, width, d_model), narrow),
            jax.ShapeDtypeStruct((parts, left, width, rows), narrow),
            jax.ShapeDtypeStruct((experts, d_model), narrow),
            jax.ShapeDtypeStruct((3, experts, 1, inner), jnp.float32),
        ),
        in_specs=[any_space] * 5,
        out_specs=(any_space,) * 5 + (pl.BlockSpec(memory_space=pltpu.VMEM),),
        scratch_shapes=[
            pltpu.VMEM((2, rows, inner), jnp.float32),
            pltpu.VMEM((2, rows, inner), jnp.float32),
            pltpu.VMEM((2, inner, rows), jnp.float32),
            pltpu.VMEM((3, 2, inner, rows), narrow),
            pltpu.VMEM((inner, LANES), jnp.float32),
            pltpu.VMEM((3, experts, parts, 1, inner), jnp.float32),
            pltpu.VMEM((experts, rows), jnp.float32),
            pltpu.VMEM((1, rows), jnp.float32),
            pltpu.VMEM((experts, d_model), narrow),
            dma((3, 2)),
            dma((3, parts - 1)),
            dma((3, experts, parts)),
            dma((3, 2, parts - 1)),
            dma((3, experts, parts)),
            dma((3, 2)),
            dma((2, parts)),
            dma((2,)),
            dma((parts - 1,)),
            dma((parts,)),
            dma,
        ],
        compiler_params=pltpu.CompilerParams(collective_id=0, has_side_effects=True),
        name="exchange",
    )(gate, up, down, weight, gain)


def spread_kernel(strip, out, send_sem, recv_sem, own_sem):
    banks = out.shape[0]
    me = lax.axis_index("bank")
    peers = [lax.rem(me + k, banks) for k in range(1, banks)]

    def copy(k, sender):
        return pltpu.make_async_remote_copy(
            src_ref=strip,
            dst_ref=out.at[sender],
            send_sem=send_sem.at[k],
            recv_sem=recv_sem.at[sender],
            device_id={"bank": peers[k]},
            device_id_type=MESH,
        )

    own = pltpu.make_async_copy(strip, out.at[me], own_sem)
    own.start()
    barrier = pltpu.get_barrier_semaphore()
    for peer in peers:
        pl.semaphore_signal(barrier, inc=1, device_id={"bank": peer}, device_id_type=MESH)
    pl.semaphore_wait(barrier, banks - 1)
    for k in range(banks - 1):
        copy(k, me).start()
    for k in range(banks - 1):
        copy(k, me).wait_send()
        copy(k, peers[k]).wait_recv()
    own.wait()


def spread(banks, strip):
    dma = pltpu.SemaphoreType.DMA
    return pl.pallas_call(
        spread_kernel,
        out_shape=jax.ShapeDtypeStruct((banks, *strip.shape), strip.dtype),
        in_specs=[pl.BlockSpec(memory_space=pl.ANY)],
        out_specs=pl.BlockSpec(memory_space=pl.ANY),
        scratch_shapes=[dma((banks - 1,)), dma((banks,)), dma],
        compiler_params=pltpu.CompilerParams(collective_id=1, has_side_effects=True),
        cost_estimate=pl.CostEstimate(
            flops=strip.size, bytes_accessed=4 * banks * strip.size, transcendentals=0
        ),
        name="spread",
    )(strip)


def place_kernel(gate, up, down, router, *refs):
    arrays, stages, (into, out_of) = (gate, up, down, router), refs[4:8], refs[8:]
    pieces = [
        (source.at[e], stage.at[e], result.at[e])
        for source, result, stage in zip(arrays, refs[:4], stages)
        for e in range(source.shape[0])
    ]
    loads = [
        pltpu.make_async_copy(source, stage, into.at[i])
        for i, (source, stage, _) in enumerate(pieces)
    ]
    stores = [
        pltpu.make_async_copy(stage, result, out_of.at[i])
        for i, (_, stage, result) in enumerate(pieces)
    ]
    for copy in loads:
        copy.start()
    for load, store in zip(loads, stores):
        load.wait()
        store.start()
    for copy in stores:
        copy.wait()


def place(*arrays):
    gate, up, down, router = arrays
    results = (gate, up, gate, router)
    pieces = sum(array.shape[0] for array in arrays)
    any_space = pl.BlockSpec(memory_space=pl.ANY)
    moved = sum(array.size for array in arrays)
    return pl.pallas_call(
        place_kernel,
        out_shape=tuple(jax.ShapeDtypeStruct(r.shape, r.dtype) for r in results),
        in_specs=[any_space] * 4,
        out_specs=(any_space,) * 4,
        scratch_shapes=[pltpu.VMEM(array.shape, array.dtype) for array in arrays]
        + [pltpu.SemaphoreType.DMA((pieces,))] * 2,
        cost_estimate=pl.CostEstimate(flops=moved, bytes_accessed=4 * moved, transcendentals=0),
        name="place",
    )(*arrays)


def fill_kernel(blocks, _, out, sem):
    parts, left, _, rows = blocks.shape
    kept = out.shape[0] - left
    copies = [
        pltpu.make_async_copy(
            blocks.at[p, e], out.at[kept + e, :, pl.ds(p * rows, rows)], sem.at[p, e]
        )
        for p in range(parts)
        for e in range(left)
    ]
    for copy in copies:
        copy.start()
    for copy in copies:
        copy.wait()


def fill(blocks, partial):
    parts, left = blocks.shape[:2]
    any_space = pl.BlockSpec(memory_space=pl.ANY)
    return pl.pallas_call(
        fill_kernel,
        out_shape=jax.ShapeDtypeStruct(partial.shape, partial.dtype),
        in_specs=[pl.BlockSpec(memory_space=pltpu.VMEM), any_space],
        out_specs=any_space,
        scratch_shapes=[pltpu.SemaphoreType.DMA((parts, left))],
        input_output_aliases={1: 0},
        compiler_params=pltpu.CompilerParams(vmem_limit_bytes=1 << 20),
        name="fill",
    )(blocks, partial)


def local(parts, banks, master_gate, master_up, master_down, router_weight, router_gain):
    experts, rows, inner = master_gate.shape
    d_model, width = rows * parts, inner // parts
    kept = experts - max(experts // 4, 1)
    *got, cut, strip, scales = exchange(
        parts, kept, master_gate, master_up, master_down,
        router_weight.T, router_gain.reshape(1, rows),
    )
    late = lax.all_to_all(cut, "zero", split_axis=0, concat_axis=0, tiled=True)
    final_gate, final_up, final_down, router = place(*got, spread(banks, strip))
    final_down = fill(late, final_down)
    own = lax.dynamic_slice_in_dim(scales[:, :, 0], lax.axis_index("zero") * width, width, axis=2)
    return (
        final_gate.transpose(0, 2, 1),
        final_up.transpose(0, 2, 1),
        final_down,
        own[GATE],
        own[UP],
        own[DOWN],
        router.reshape(-1, d_model).T,
    )


def solution(mesh):
    placed = (
        P("bank", "zero", None),
        P("bank", "zero", None),
        P("bank", None, "zero"),
        P("zero", "bank"),
        P("zero"),
    )
    parts, banks = mesh.shape["zero"], mesh.shape["bank"]
    return jax.shard_map(
        lambda *arrays: local(parts, banks, *arrays),
        mesh=mesh,
        in_specs=placed,
        out_specs=(
            P("bank", None, "zero"),
            P("bank", None, "zero"),
            P("bank", "zero", None),
            P("bank", "zero"),
            P("bank", "zero"),
            P("bank", "zero"),
            P(),
        ),
        check_vma=False,
    )
```

```python
import functools
import math

import jax
import jax.numpy as jnp
from jax import lax
from jax.experimental import pallas as pl
from jax.experimental.pallas import tpu as pltpu
from jax.sharding import PartitionSpec as P

LANES = 128
DOWN, GATE, UP = range(3)
MESH = pl.DeviceIdType.MESH


def span(index, size):
    return pl.ds(pl.multiple_of(index * size, size), size)


def row_sums_across(wide, put):
    def one(j, _):
        put(j, jnp.sum(jnp.abs(wide[:, span(j, LANES)]), axis=0, keepdims=True))
        return 0

    lax.fori_loop(0, wide.shape[1] // LANES, one, 0)


def row_sums_along(wide, put):
    def one(j, _):
        block = jnp.abs(wide[span(j, LANES), :])
        total = block[:, :LANES]
        for k in range(1, block.shape[1] // LANES):
            total = total + block[:, k * LANES : (k + 1) * LANES]
        put(j, jnp.sum(total.T, axis=0, keepdims=True))
        return 0

    lax.fori_loop(0, wide.shape[0] // LANES, one, 0, unroll=True)


def exchange_kernel(
    parts,
    kept,
    gate,
    up,
    down,
    weight,
    gain,
    out_gate,
    out_up,
    out_down,
    *refs,
):
    cut, (out_router, scales, *refs) = refs[:parts], refs[parts:]
    (
        wide_gate,
        wide_up,
        wide_down,
        narrow,
        columns_of,
        sums,
        weight_now,
        gain_now,
        strip,
        load_sem,
        sum_send,
        sum_recv,
        data_send,
        data_recv,
        own_sem,
        cut_sem,
        router_load,
        part_send,
        part_recv,
        strip_send,
        strip_recv,
        strip_own,
    ) = refs
    me, here = lax.axis_index("zero"), lax.axis_index("bank")
    experts, rows, inner = gate.shape
    width = inner // parts
    chunk = math.gcd(width, 32)
    d_model = rows * parts
    source = {DOWN: down, GATE: gate, UP: up}
    wide = {DOWN: wide_down, GATE: wide_gate, UP: wide_up}
    result = {DOWN: out_down, GATE: out_gate, UP: out_up}
    banks = out_router.shape[0]
    peers = [lax.rem(me + k, parts) for k in range(1, parts)]
    others = [lax.rem(here + k, banks) for k in range(1, banks)]

    def load(m, e):
        slot = lax.rem(e, 2)
        return pltpu.make_async_copy(source[m].at[e], wide[m].at[slot], load_sem.at[m, slot])

    def sum_copy(m, e, k, sender):
        return pltpu.make_async_remote_copy(
            src_ref=sums.at[m, e, sender],
            dst_ref=sums.at[m, e, sender],
            send_sem=sum_send.at[m, k],
            recv_sem=sum_recv.at[m, e, sender],
            device_id={"zero": peers[k]},
            device_id_type=MESH,
        )

    def block_copy(m, e, k, sender):
        slot = lax.rem(e, 2)
        return pltpu.make_async_remote_copy(
            src_ref=narrow.at[m, slot, span(peers[k], width), :],
            dst_ref=result[m].at[e, :, span(sender, rows)],
            send_sem=data_send.at[m, slot, k],
            recv_sem=data_recv.at[m, e, sender],
            device_id={"zero": peers[k]},
            device_id_type=MESH,
        )

    def own_copy(m, e):
        slot = lax.rem(e, 2)
        return pltpu.make_async_copy(
            narrow.at[m, slot, span(me, width), :],
            result[m].at[e, :, span(me, rows)],
            own_sem.at[m, slot],
        )

    def cut_copy(e, p):
        slot = lax.rem(e, 2)
        return pltpu.make_async_copy(
            narrow.at[DOWN, slot, span(lax.rem(me + p, parts), width), :],
            cut[p].at[e - kept],
            cut_sem.at[slot, p],
        )

    def begin(m, e, ready=lambda: None):
        load(m, e).wait()
        slot = lax.rem(e, 2)
        if m != UP:
            pl.when(e < 2)(lambda: load(m + 1, e).start())
        elif experts > 1:
            pl.when(e < 1)(lambda: load(DOWN, e + 1).start())

        def put(j, value):
            sums[m, e, me, :, span(j, LANES)] = value

        (row_sums_along if m == DOWN else row_sums_across)(wide[m].at[slot], put)
        ready()
        for k in range(parts - 1):
            sum_copy(m, e, k, me).start()

    def sent(m, e):
        def remote():
            for k in range(parts - 1):
                block_copy(m, e, k, me).wait_send()
            own_copy(m, e).wait()

        if m != DOWN:
            remote()
            return
        pl.when(e < kept)(remote)

        @pl.when(e >= kept)
        def _():
            for p in range(parts):
                cut_copy(e, p).wait()

    def finish(m, e):
        slot = lax.rem(e, 2)
        for k in range(parts - 1):
            sum_copy(m, e, k, me).wait_send()
            sum_copy(m, e, k, peers[k]).wait_recv()
        pl.when(e >= 2)(lambda: sent(m, e - 2))
        wide_now, narrow_now = wide[m].at[slot], narrow.at[m, slot]

        def inverse_of(columns):
            total = sums[m, e, 0, :, columns]
            for p in range(1, parts):
                total = total + sums[m, e, p, :, columns]
            scale = total / d_model
            scales[m, e, :, columns] = scale
            return 1.0 / scale

        if m == DOWN:

            def by_row(j, _):
                columns = span(j, LANES)
                inverse = jnp.broadcast_to(inverse_of(columns), (LANES, LANES))
                columns_of[columns, :] = inverse.T
                return 0

            lax.fori_loop(0, inner // LANES, by_row, 0, unroll=True)

            def scaled(p):
                def one(c, _):
                    at = pl.ds(pl.multiple_of(p * width + c * chunk, chunk), chunk)
                    inverse = columns_of[at, :]
                    for i in range(rows // LANES):
                        lanes = pl.ds(i * LANES, LANES)
                        narrow_now[at, lanes] = (wide_now[at, lanes] * inverse).astype(jnp.bfloat16)
                    return 0

                lax.fori_loop(0, width // chunk, one, 0, unroll=True)

            for k in range(parts - 1):
                scaled(peers[k])
                pl.when(e < kept)(lambda: block_copy(DOWN, e, k, me).start())
            scaled(me)
            pl.when(e < kept)(lambda: own_copy(DOWN, e).start())

            @pl.when(e >= kept)
            def _():
                for p in range(parts):
                    cut_copy(e, p).start()

        else:

            def one(j, _):
                columns = span(j, LANES)
                inverse = inverse_of(columns)
                for i in range(rows // LANES):
                    at = pl.ds(i * LANES, LANES)
                    block = wide_now[at, columns] * inverse
                    narrow_now[columns, at] = block.T.astype(jnp.bfloat16)
                return 0

            lax.fori_loop(0, inner // LANES, one, 0)
            for k in range(parts - 1):
                block_copy(m, e, k, me).start()
            own_copy(m, e).start()
        pl.when(e + 2 < experts)(lambda: load(m, e + 2).start())

    def part_copy(k, sender):
        return pltpu.make_async_remote_copy(
            src_ref=strip.at[:, span(sender, rows)],
            dst_ref=strip.at[:, span(sender, rows)],
            send_sem=part_send.at[k],
            recv_sem=part_recv.at[sender],
            device_id={"zero": peers[k]},
            device_id_type=MESH,
        )

    def strip_copy(k, sender):
        return pltpu.make_async_remote_copy(
            src_ref=strip,
            dst_ref=out_router.at[sender],
            send_sem=strip_send.at[k],
            recv_sem=strip_recv.at[sender],
            device_id={"bank": others[k]},
            device_id_type=MESH,
        )

    own_strip = pltpu.make_async_copy(strip, out_router.at[here], strip_own)
    router_loads = [
        pltpu.make_async_copy(weight, weight_now, router_load.at[0]),
        pltpu.make_async_copy(gain, gain_now, router_load.at[1]),
    ]

    load(DOWN, 0).start()
    for copy in router_loads:
        copy.start()
    barrier = pltpu.get_barrier_semaphore()
    for peer in peers:
        pl.semaphore_signal(barrier, inc=1, device_id={"zero": peer}, device_id_type=MESH)
    for other in others:
        pl.semaphore_signal(barrier, inc=1, device_id={"bank": other}, device_id_type=MESH)
    begin(DOWN, 0, lambda: pl.semaphore_wait(barrier, parts + banks - 2))
    begin(GATE, 0)
    for copy in router_loads:
        copy.wait()
    strip[:, span(me, rows)] = (weight_now[...] * gain_now[...]).astype(jnp.bfloat16)
    for k in range(parts - 1):
        part_copy(k, me).start()

    def step(e, _):
        more = e + 1 < experts
        finish(DOWN, e)
        begin(UP, e)
        pl.when(more)(lambda: begin(DOWN, e + 1))
        finish(GATE, e)
        pl.when(more)(lambda: begin(GATE, e + 1))
        finish(UP, e)

        @pl.when(e == experts // 2)
        def _():
            for k in range(parts - 1):
                part_copy(k, peers[k]).wait_recv()
            for k in range(banks - 1):
                strip_copy(k, here).start()
            own_strip.start()

        return 0

    lax.fori_loop(0, experts, step, 0)

    for m in (DOWN, GATE, UP):
        for e in range(max(experts - 2, 0), experts):
            sent(m, jnp.int32(e))

    def arrived(e, _):
        for k in range(parts - 1):
            for m in (GATE, UP):
                block_copy(m, e, k, peers[k]).wait_recv()

            @pl.when(e < kept)
            def _():
                block_copy(DOWN, e, k, peers[k]).wait_recv()

        return 0

    lax.fori_loop(0, experts, arrived, 0)
    for k in range(parts - 1):
        part_copy(k, me).wait_send()
    for k in range(banks - 1):
        strip_copy(k, here).wait_send()
        strip_copy(k, others[k]).wait_recv()
    own_strip.wait()


def exchange(parts, banks, kept, gate, up, down, weight, gain):
    experts, rows, inner = gate.shape
    width, d_model = inner // parts, rows * parts
    left = experts - kept
    any_space = pl.BlockSpec(memory_space=pl.ANY)
    narrow = jnp.bfloat16
    dma = pltpu.SemaphoreType.DMA
    return pl.pallas_call(
        functools.partial(exchange_kernel, parts, kept),
        out_shape=(
            jax.ShapeDtypeStruct((experts, width, d_model), narrow),
            jax.ShapeDtypeStruct((experts, width, d_model), narrow),
            jax.ShapeDtypeStruct((kept, width, d_model), narrow),
            *[jax.ShapeDtypeStruct((left, width, rows), narrow)] * parts,
            jax.ShapeDtypeStruct((banks, experts, d_model), narrow),
            jax.ShapeDtypeStruct((3, experts, 1, inner), jnp.float32),
        ),
        in_specs=[any_space] * 5,
        out_specs=(any_space,) * (4 + parts) + (pl.BlockSpec(memory_space=pltpu.VMEM),),
        scratch_shapes=[
            pltpu.VMEM((2, rows, inner), jnp.float32),
            pltpu.VMEM((2, rows, inner), jnp.float32),
            pltpu.VMEM((2, inner, rows), jnp.float32),
            pltpu.VMEM((3, 2, inner, rows), narrow),
            pltpu.VMEM((inner, LANES), jnp.float32),
            pltpu.VMEM((3, experts, parts, 1, inner), jnp.float32),
            pltpu.VMEM((experts, rows), jnp.float32),
            pltpu.VMEM((1, rows), jnp.float32),
            pltpu.VMEM((experts, d_model), narrow),
            dma((3, 2)),
            dma((3, parts - 1)),
            dma((3, experts, parts)),
            dma((3, 2, parts - 1)),
            dma((3, experts, parts)),
            dma((3, 2)),
            dma((2, parts)),
            dma((2,)),
            dma((parts - 1,)),
            dma((parts,)),
            dma((banks - 1,)),
            dma((banks,)),
            dma,
        ],
        compiler_params=pltpu.CompilerParams(collective_id=0, has_side_effects=True),
        name="exchange",
    )(gate, up, down, weight, gain)


def place_kernel(
    parts, gate, up, down, router, scales,
    out_gate, out_up, out_down, out_router, own_gate, own_up, own_down,
    stage_gate, stage_up, stage_down, stage_router, into, out_of,
):
    pieces = [
        (source.at[e], stage.at[e], result.at[e])
        for source, stage, result in (
            (gate, stage_gate, out_gate),
            (up, stage_up, out_up),
            (down, stage_down, out_down),
        )
        for e in range(source.shape[0])
    ] + [(router, stage_router, out_router)]
    loads = [
        pltpu.make_async_copy(source, stage, into.at[i])
        for i, (source, stage, _) in enumerate(pieces)
    ]
    stores = [
        pltpu.make_async_copy(stage, result, out_of.at[i])
        for i, (_, stage, result) in enumerate(pieces)
    ]
    for copy in loads:
        copy.start()
    for load, store in zip(loads, stores):
        load.wait()
        store.start()
    inner, width = scales.shape[3], own_gate.shape[1]
    shift = lax.rem(inner - lax.axis_index("zero") * width, inner)
    for m, own in ((GATE, own_gate), (UP, own_up), (DOWN, own_down)):
        for e in range(own.shape[0]):
            own[e : e + 1, :] = pltpu.roll(scales[m, e], shift, 1)[:, :width]
    for copy in stores:
        copy.wait()


def place(parts, gate, up, down, router, scales):
    arrays = (gate, up, down, router)
    results = (gate, up, gate, router)
    experts, inner = scales.shape[1], scales.shape[3]
    own = jax.ShapeDtypeStruct((experts, inner // parts), scales.dtype)
    pieces = gate.shape[0] + up.shape[0] + down.shape[0] + 1
    any_space, vmem = pl.BlockSpec(memory_space=pl.ANY), pl.BlockSpec(memory_space=pltpu.VMEM)
    moved = sum(array.size for array in arrays)
    return pl.pallas_call(
        functools.partial(place_kernel, parts),
        out_shape=tuple(jax.ShapeDtypeStruct(r.shape, r.dtype) for r in results) + (own,) * 3,
        in_specs=[any_space] * 4 + [vmem],
        out_specs=(any_space,) * 4 + (vmem,) * 3,
        scratch_shapes=[pltpu.VMEM(array.shape, array.dtype) for array in arrays]
        + [pltpu.SemaphoreType.DMA((pieces,))] * 2,
        cost_estimate=pl.CostEstimate(flops=moved, bytes_accessed=4 * moved, transcendentals=0),
        name="place",
    )(gate, up, down, router, scales)


def fill_kernel(parts, *refs):
    blocks, out, sem = refs[:parts], refs[parts + 1], refs[parts + 2]
    me = lax.axis_index("zero")
    left, _, rows = blocks[0].shape
    kept = out.shape[0] - left
    copies = [
        pltpu.make_async_copy(
            blocks[k].at[e],
            out.at[kept + e, :, span(lax.rem(me + parts - k, parts), rows)],
            sem.at[k, e],
        )
        for k in range(parts)
        for e in range(left)
    ]
    for copy in copies:
        copy.start()
    for copy in copies:
        copy.wait()


def fill(blocks, partial):
    parts, left = len(blocks), blocks[0].shape[0]
    any_space = pl.BlockSpec(memory_space=pl.ANY)
    return pl.pallas_call(
        functools.partial(fill_kernel, parts),
        out_shape=jax.ShapeDtypeStruct(partial.shape, partial.dtype),
        in_specs=[pl.BlockSpec(memory_space=pltpu.VMEM)] * parts + [any_space],
        out_specs=any_space,
        scratch_shapes=[pltpu.SemaphoreType.DMA((parts, left))],
        input_output_aliases={parts: 0},
        compiler_params=pltpu.CompilerParams(vmem_limit_bytes=1 << 20),
        name="fill",
    )(*blocks, partial)


def local(parts, banks, master_gate, master_up, master_down, router_weight, router_gain):
    experts, rows, inner = master_gate.shape
    d_model = rows * parts
    kept = experts - max(experts // 4, 1)
    got_gate, got_up, got_down, own_cut, *cuts, router, scales = exchange(
        parts, banks, kept, master_gate, master_up, master_down,
        router_weight.T, router_gain.reshape(1, rows),
    )
    late = [
        lax.ppermute(cut, "zero", [(p, (p + k) % parts) for p in range(parts)])
        for k, cut in enumerate(cuts, 1)
    ]
    final_gate, final_up, final_down, router, *own = place(
        parts, got_gate, got_up, got_down, router, scales
    )
    final_down = fill([own_cut, *late], final_down)
    return (
        final_gate.transpose(0, 2, 1),
        final_up.transpose(0, 2, 1),
        final_down,
        *own,
        router.reshape(-1, d_model).T,
    )


def solution(mesh):
    placed = (
        P("bank", "zero", None),
        P("bank", "zero", None),
        P("bank", None, "zero"),
        P("zero", "bank"),
        P("zero"),
    )
    parts, banks = mesh.shape["zero"], mesh.shape["bank"]
    return jax.shard_map(
        lambda *arrays: local(parts, banks, *arrays),
        mesh=mesh,
        in_specs=placed,
        out_specs=(
            P("bank", None, "zero"),
            P("bank", None, "zero"),
            P("bank", "zero", None),
            P("bank", "zero"),
            P("bank", "zero"),
            P("bank", "zero"),
            P(),
        ),
        check_vma=False,
    )
```
